32 devices in a mesh: dp: 4 (over z), tp: 8 (over y, x, core).
Axes of the slice: x: 2, y: 2, z: 4, core: 2. Of those that a mesh axis runs over, the one named last changes fastest.
Arguments:
- resid_in: bfloat16 [512, 6144], P('dp'), parts along dimension 0
- positions: int32 [512], P('dp'), parts along dimension 0
- k_cache: bfloat16 [512, 128, 8, 128], P('dp', None, 'tp'), parts along dimension 0
- v_cache: bfloat16 [512, 128, 8, 128], P('dp', None, 'tp'), parts along dimension 0
- gain_attn: bfloat16 [6144], replicated
- w_query: bfloat16 [6144, 6144], P(None, 'tp')
- w_key: bfloat16 [6144, 1024], P(None, 'tp')
- w_value: bfloat16 [6144, 1024], P(None, 'tp')
- w_out: bfloat16 [6144, 6144], P('tp')
- gain_mlp: bfloat16 [6144], replicated
- w_gate: bfloat16 [6144, 16384], P(None, 'tp')
- w_up: bfloat16 [6144, 16384], P(None, 'tp')
- w_down: bfloat16 [16384, 6144], P('tp')
Outputs:
- output 1: bfloat16 [512, 6144], P('dp'), parts along dimension 0
- output 2: bfloat16 [512, 128, 8, 128], P('dp', None, 'tp'), parts along dimension 0
- output 3: bfloat16 [512, 128, 8, 128], P('dp', None, 'tp'), parts along dimension 0
There are 4 independent parts. The reference program is written for one: setup_inputs(seed, part) draws one part's arguments, and reference() takes and returns one part's arrays. A program takes and returns all parts, laid end to end along the dimension named above; an argument that names none is the same for every part.
All inputs are finite; a program needn't handle non-finite values.
Results may differ from the reference program's by a relative error of at most 0.0104617.
Values sent between devices are 32-bit elements.
A program may use at most 1 GiB of HBM per device.

```python
import math
import jax
import jax.numpy as jnp
from jax import lax

BATCH_PART = 128
CACHE_LEN = 128
MODEL_DIM = 6144
Q_HEADS = 48
KV_HEADS = 8
HEAD_DIM = 128
FFN_DIM = 16384

EPS = 1e-5
ROPE_THETA = 500000.0
ROPE_FACTOR = 8.0
LOW_FACTOR = 1.0
HIGH_FACTOR = 4.0
ORIG_CTX = 8192.0


def setup_inputs(seed: int = 0, part: int = 0) -> dict:
    part_keys = jax.random.split(jax.random.fold_in(jax.random.key(seed), part), 6)
    weight_keys = jax.random.split(jax.random.key(seed + 1), 11)
    log_len = int(math.log2(CACHE_LEN))
    dim_scale = 1.0 / math.sqrt(MODEL_DIM)
    out_scale = 1.0 / math.sqrt(Q_HEADS * HEAD_DIM)
    ffn_scale = 1.0 / math.sqrt(FFN_DIM)
    q_width = Q_HEADS * HEAD_DIM
    kv_width = KV_HEADS * HEAD_DIM
    resid_in = jax.random.normal(part_keys[0], (BATCH_PART, MODEL_DIM), jnp.float32)
    exponent = jax.random.randint(part_keys[1], (BATCH_PART,), 0, log_len + 1, dtype=jnp.int32)
    upper_bound = jnp.left_shift(jnp.ones((BATCH_PART,), jnp.int32), exponent)
    positions = jax.random.randint(part_keys[2], (BATCH_PART,), 0, upper_bound, dtype=jnp.int32)
    positions = positions.at[0].set(CACHE_LEN - 1).at[1].set(0)
    cache_shape = (BATCH_PART, CACHE_LEN, KV_HEADS, HEAD_DIM)
    k_cache = jax.random.normal(part_keys[3], cache_shape, jnp.float32)
    v_mean = 0.7 * jax.random.normal(part_keys[4], (BATCH_PART, 1, KV_HEADS, HEAD_DIM), jnp.float32)
    v_cache = v_mean + jax.random.normal(part_keys[5], cache_shape, jnp.float32)
    gain_attn = 1.0 + 0.3 * jax.random.normal(weight_keys[0], (MODEL_DIM,), jnp.float32)
    w_query = jax.random.normal(weight_keys[1], (MODEL_DIM, q_width), jnp.float32) * dim_scale
    w_key = jax.random.normal(weight_keys[2], (MODEL_DIM, kv_width), jnp.float32) * dim_scale
    w_value = jax.random.normal(weight_keys[3], (MODEL_DIM, kv_width), jnp.float32) * dim_scale
    w_out = jax.random.normal(weight_keys[4], (q_width, MODEL_DIM), jnp.float32) * out_scale
    gain_mlp = 1.0 + 0.3 * jax.random.normal(weight_keys[5], (MODEL_DIM,), jnp.float32)
    w_gate = jax.random.normal(weight_keys[6], (MODEL_DIM, FFN_DIM), jnp.float32) * dim_scale
    w_up = jax.random.normal(weight_keys[7], (MODEL_DIM, FFN_DIM), jnp.float32) * dim_scale
    w_down = jax.random.normal(weight_keys[8], (FFN_DIM, MODEL_DIM), jnp.float32) * ffn_scale
    return dict(resid_in=resid_in.astype(jnp.bfloat16), positions=positions,
                k_cache=k_cache.astype(jnp.bfloat16), v_cache=v_cache.astype(jnp.bfloat16),
                gain_attn=gain_attn.astype(jnp.bfloat16), w_query=w_query.astype(jnp.bfloat16),
                w_key=w_key.astype(jnp.bfloat16), w_value=w_value.astype(jnp.bfloat16),
                w_out=w_out.astype(jnp.bfloat16), gain_mlp=gain_mlp.astype(jnp.bfloat16),
                w_gate=w_gate.astype(jnp.bfloat16), w_up=w_up.astype(jnp.bfloat16),
                w_down=w_down.astype(jnp.bfloat16))


def rms_norm(rows_in, gain):
    rows_f = rows_in.astype(jnp.float32)
    mean_sq = jnp.mean(rows_f * rows_f, axis=-1, keepdims=True)
    return (rows_f * lax.rsqrt(mean_sq + EPS) * gain.astype(jnp.float32)).astype(jnp.bfloat16)


def rope_tables(positions, head_dim):
    half_dim = head_dim // 2
    exponents = jnp.arange(half_dim, dtype=jnp.float32) * (2.0 / head_dim)
    inv_freq = 1.0 / jnp.power(ROPE_THETA, exponents)
    wavelen = (2.0 * math.pi) / inv_freq
    smooth = (ORIG_CTX / wavelen - LOW_FACTOR) / (HIGH_FACTOR - LOW_FACTOR)
    blended = (1.0 - smooth) * inv_freq / ROPE_FACTOR + smooth * inv_freq
    inv_freq = jnp.where(wavelen < ORIG_CTX / HIGH_FACTOR, inv_freq,
                         jnp.where(wavelen > ORIG_CTX / LOW_FACTOR, inv_freq / ROPE_FACTOR, blended))
    angles = positions.astype(jnp.float32)[:, None] * inv_freq[None, :]
    return jnp.cos(angles), jnp.sin(angles)


def apply_rope(vectors, cos_t, sin_t):
    half_dim = vectors.shape[-1] // 2
    lower_half = vectors[..., :half_dim]
    upper_half = vectors[..., half_dim:]
    cos_b = cos_t[:, None, :]
    sin_b = sin_t[:, None, :]
    return jnp.concatenate([lower_half * cos_b - upper_half * sin_b,
                            upper_half * cos_b + lower_half * sin_b], axis=-1)


def reference(resid_in, positions, k_cache, v_cache, gain_attn, w_query, w_key, w_value,
              w_out, gain_mlp, w_gate, w_up, w_down):
    group_size = Q_HEADS // KV_HEADS
    n_seqs = resid_in.shape[0]
    normed = rms_norm(resid_in, gain_attn)
    queries = jnp.dot(normed, w_query, preferred_element_type=jnp.float32).astype(jnp.bfloat16)
    key_new = jnp.dot(normed, w_key, preferred_element_type=jnp.float32).astype(jnp.bfloat16)
    value_new = jnp.dot(normed, w_value, preferred_element_type=jnp.float32).astype(jnp.bfloat16)
    cos_t, sin_t = rope_tables(positions, HEAD_DIM)
    queries = apply_rope(queries.reshape(n_seqs, Q_HEADS, HEAD_DIM).astype(jnp.float32), cos_t, sin_t)
    queries = queries.astype(jnp.bfloat16)
    key_new = apply_rope(key_new.reshape(n_seqs, KV_HEADS, HEAD_DIM).astype(jnp.float32), cos_t, sin_t)
    key_new = key_new.astype(jnp.bfloat16)
    value_new = value_new.reshape(n_seqs, KV_HEADS, HEAD_DIM)
    slot_hit = (jnp.arange(CACHE_LEN)[None, :] == positions[:, None])[:, :, None, None]
    k_full = jnp.where(slot_hit, key_new[:, None], k_cache)
    v_full = jnp.where(slot_hit, value_new[:, None], v_cache)
    scale = 1.0 / math.sqrt(HEAD_DIM)

    def one_seq(seq_items):
        q_seq, k_seq, v_seq, pos_seq = seq_items
        q_grp = q_seq.reshape(KV_HEADS, group_size, HEAD_DIM).astype(jnp.float32)
        scores = jnp.einsum('kgd,skd->kgs', q_grp, k_seq.astype(jnp.float32)) * scale
        valid = jnp.arange(CACHE_LEN) <= pos_seq
        scores = jnp.where(valid[None, None, :], scores, -jnp.inf)
        attn_prob = jax.nn.softmax(scores, axis=-1).astype(jnp.bfloat16)
        attn_seq = jnp.einsum('kgs,skd->kgd', attn_prob.astype(jnp.float32), v_seq.astype(jnp.float32))
        return attn_seq.astype(jnp.bfloat16).reshape(Q_HEADS * HEAD_DIM)

    attn_out = lax.map(one_seq, (queries, k_full, v_full, positions))
    y_full = jnp.dot(attn_out, w_out, preferred_element_type=jnp.float32)
    resid_mid = (resid_in.astype(jnp.float32) + y_full).astype(jnp.bfloat16)
    normed_mlp = rms_norm(resid_mid, gain_mlp)
    gate_proj = jnp.dot(normed_mlp, w_gate, preferred_element_type=jnp.float32).astype(jnp.bfloat16)
    up_proj = jnp.dot(normed_mlp, w_up, preferred_element_type=jnp.float32).astype(jnp.bfloat16)
    hidden = (jax.nn.silu(gate_proj.astype(jnp.float32)) * up_proj.astype(jnp.float32)).astype(jnp.bfloat16)
    z_full = jnp.dot(hidden, w_down, preferred_element_type=jnp.float32)
    resid_out = (resid_mid.astype(jnp.float32) + z_full).astype(jnp.bfloat16)
    return resid_out, k_full, v_full
```

```python
import math
import jax
import jax.numpy as jnp
from jax import lax
from jax.experimental import pallas as pl
from jax.experimental.pallas import tpu as pltpu
from jax.sharding import PartitionSpec as P

EPS = 1e-5
ROPE_THETA = 500000.0
ROPE_FACTOR = 8.0
LOW_FACTOR = 1.0
HIGH_FACTOR = 4.0
ORIG_CTX = 8192.0


def rms_norm(rows_in, gain):
    rows_f = rows_in.astype(jnp.float32)
    mean_sq = jnp.mean(rows_f * rows_f, axis=-1, keepdims=True)
    return (rows_f * lax.rsqrt(mean_sq + EPS) * gain.astype(jnp.float32)).astype(jnp.bfloat16)


def rope_tables(positions, head_dim):
    half_dim = head_dim // 2
    exponents = jnp.arange(half_dim, dtype=jnp.float32) * (2.0 / head_dim)
    inv_freq = 1.0 / jnp.power(ROPE_THETA, exponents)
    wavelen = (2.0 * math.pi) / inv_freq
    smooth = (ORIG_CTX / wavelen - LOW_FACTOR) / (HIGH_FACTOR - LOW_FACTOR)
    blended = (1.0 - smooth) * inv_freq / ROPE_FACTOR + smooth * inv_freq
    inv_freq = jnp.where(wavelen < ORIG_CTX / HIGH_FACTOR, inv_freq,
                         jnp.where(wavelen > ORIG_CTX / LOW_FACTOR, inv_freq / ROPE_FACTOR, blended))
    angles = positions.astype(jnp.float32)[:, None] * inv_freq[None, :]
    return jnp.cos(angles), jnp.sin(angles)


def apply_rope(vectors, cos_t, sin_t):
    half_dim = vectors.shape[-1] // 2
    lower_half = vectors[..., :half_dim]
    upper_half = vectors[..., half_dim:]
    cos_b = cos_t[:, None, :]
    sin_b = sin_t[:, None, :]
    return jnp.concatenate([lower_half * cos_b - upper_half * sin_b,
                            upper_half * cos_b + lower_half * sin_b], axis=-1)


def attention_block(resid_in, positions, k_cache, v_cache, gain_attn, w_query, w_key, w_value):
    n_seqs = resid_in.shape[0]
    cache_len = k_cache.shape[1]
    kv_heads = k_cache.shape[2]
    head_dim = k_cache.shape[3]
    group_size = w_query.shape[1] // (kv_heads * head_dim)
    normed = rms_norm(resid_in, gain_attn)
    queries = jnp.dot(normed, w_query, preferred_element_type=jnp.float32).astype(jnp.bfloat16)
    key_new = jnp.dot(normed, w_key, preferred_element_type=jnp.float32).astype(jnp.bfloat16)
    value_new = jnp.dot(normed, w_value, preferred_element_type=jnp.float32).astype(jnp.bfloat16)
    cos_t, sin_t = rope_tables(positions, head_dim)
    queries = apply_rope(queries.reshape(n_seqs, kv_heads * group_size, head_dim).astype(jnp.float32), cos_t, sin_t)
    queries = queries.astype(jnp.bfloat16).reshape(n_seqs, kv_heads, group_size, head_dim)
    key_new = apply_rope(key_new.reshape(n_seqs, kv_heads, head_dim).astype(jnp.float32), cos_t, sin_t)
    key_new = key_new.astype(jnp.bfloat16)
    value_new = value_new.reshape(n_seqs, kv_heads, head_dim)
    slot_iota = lax.broadcasted_iota(jnp.int32, (n_seqs, cache_len), 1)
    slot_hit = (slot_iota == positions[:, None])[:, :, None, None]
    k_full = jnp.where(slot_hit, key_new[:, None], k_cache)
    v_full = jnp.where(slot_hit, value_new[:, None], v_cache)
    scores = jnp.einsum('bkgd,bskd->bkgs', queries, k_full, preferred_element_type=jnp.float32)
    scores = scores * (1.0 / math.sqrt(head_dim))
    valid = (slot_iota <= positions[:, None])[:, None, None, :]
    scores = jnp.where(valid, scores, -jnp.inf)
    attn_prob = jax.nn.softmax(scores, axis=-1).astype(jnp.bfloat16)
    attn_out = jnp.einsum('bkgs,bskd->bkgd', attn_prob, v_full, preferred_element_type=jnp.float32)
    attn_out = attn_out.astype(jnp.bfloat16).reshape(n_seqs, kv_heads * group_size * head_dim)
    return attn_out, k_full, v_full


F32 = jnp.float32
BF16 = jnp.bfloat16
REL = ((1, 1), (0, 1), (1, 0), (0, 0))
WO_SLOTS = 4
GU_SLOTS = 5
WD_SLOTS = 4
GATHER_ORDER = ((0, 3), (1, 3), (0, 1), (0, 2), (1, 1), (1, 2), (0, 0), (1, 0))


def flip(coord, do_flip):
    return 1 - coord if do_flip else coord


def tail_kernel(attn_ref, gain_ref, resid_hbm, wo_hbm, wg_hbm, wu_hbm, wd_hbm, out_hbm,
                wo_buf, wg_buf, wu_buf, wd_buf, ybuf, dbuf, r1, r2, xg, acc_g, acc_u, abuf, hbuf,
                resid_buf, obuf, stat, stat_out, gbuf, rbuf,
                wo_sem, gu_sem, wd_sem, resid_sem, out_sem, d_send, d_recv, rs_send, rs_recv,
                ag_send, ag_recv, st_send, st_recv):
    rows = attn_ref.shape[0]
    half = rows // 2
    block = wo_buf.shape[2]
    piece = block // 2
    width = 8 * block

    tp = lax.axis_index('tp')
    core = tp % 2
    x_pos = (tp // 2) % 2
    y_pos = tp // 4

    def device(flip_core, rel):
        flip_y, flip_x = rel
        return flip(y_pos, flip_y) * 4 + flip(x_pos, flip_x) * 2 + flip(core, flip_core)

    def owner(flip_core, e):
        return device(flip_core, REL[e])

    def cols(o):
        return pl.ds(pl.multiple_of(o * block, block), block)

    me = owner(0, 3)
    dev_d = owner(1, 3)
    dev_x = owner(0, 1)
    dev_y = owner(0, 2)

    def remote(src, dst, send, recv, dev):
        return pltpu.make_async_remote_copy(src_ref=src, dst_ref=dst, send_sem=send, recv_sem=recv,
                                            device_id={'tp': dev}, device_id_type=pl.DeviceIdType.MESH)

    order_cols = [(1 - t % 2, t // 2) for t in range(8)]

    def wo_copy(t):
        o = owner(*order_cols[t])
        return pltpu.make_async_copy(wo_hbm.at[:, cols(o)], wo_buf.at[t % WO_SLOTS], wo_sem.at[t % WO_SLOTS])

    def gu_copies(k):
        o = owner(*GATHER_ORDER[k])
        s = k % GU_SLOTS
        return (pltpu.make_async_copy(wg_hbm.at[cols(o), :], wg_buf.at[s], gu_sem.at[0, s]),
                pltpu.make_async_copy(wu_hbm.at[cols(o), :], wu_buf.at[s], gu_sem.at[1, s]))

    def wd_copy(t):
        o = owner(*order_cols[t])
        return pltpu.make_async_copy(wd_hbm.at[:, cols(o)], wd_buf.at[t % WD_SLOTS], wd_sem.at[t % WD_SLOTS])

    for t in range(WO_SLOTS):
        wo_copy(t).start()
    resid_copy = pltpu.make_async_copy(resid_hbm.at[:, cols(me)], resid_buf, resid_sem)
    resid_copy.start()

    barrier = pltpu.get_barrier_semaphore()
    for j in range(1, 8):
        pl.semaphore_signal(barrier, inc=1, device_id={'tp': (tp + j) % 8}, device_id_type=pl.DeviceIdType.MESH)

    for o in range(8):
        gbuf[o] = gain_ref[:, o * block:(o + 1) * block].astype(F32)

    def store_block(dc, e, res):
        for h in range(2):
            for ab in range(2):
                ybuf[dc, e, h, ab] = res[h * half:(h + 1) * half, ab * piece:(ab + 1) * piece]

    def d2d(e):
        return remote(ybuf.at[1, e], dbuf.at[e], d_send.at[e], d_recv.at[e], dev_d)

    def rs_copy(m, h):
        src, dst, dev = (
            (ybuf.at[0, 0, h, 0], r1.at[0, 0, h], dev_x),
            (ybuf.at[0, 1, h, 0], r1.at[0, 1, h], dev_x),
            (ybuf.at[0, 1, h, 1], r2.at[1, h], dev_x),
            (ybuf.at[0, 0, h, 1], r1.at[1, 0, h], dev_y),
            (ybuf.at[0, 2, h, 1], r1.at[1, 1, h], dev_y),
            (ybuf.at[0, 2, h, 0], r2.at[0, h], dev_y),
        )[m]
        return remote(src, dst, rs_send.at[m, h], rs_recv.at[m, h], dev)

    def add_partner(e):
        d2d(e).wait_recv()
        for h in range(2):
            for ab in range(2):
                ybuf[0, e, h, ab] = ybuf[0, e, h, ab] + dbuf[e, h, ab]
            if e == 0:
                rs_copy(0, h).start()
                rs_copy(3, h).start()
            if e == 1:
                rs_copy(1, h).start()
            if e == 2:
                rs_copy(4, h).start()

    def ag_copy(m, h):
        ox, oy, oxy = owner(0, 1), owner(0, 2), owner(0, 0)
        ref, dev = (
            (xg.at[me, h], dev_x),
            (xg.at[me, h], dev_y),
            (xg.at[me, h], dev_d),
            (xg.at[oy, h, 0], dev_x),
            (xg.at[ox, h, 1], dev_y),
            (xg.at[ox, h], dev_d),
            (xg.at[oy, h], dev_d),
            (xg.at[oxy, h, 0], dev_d),
            (xg.at[oxy, h, 1], dev_d),
        )[m]
        return remote(ref, ref, ag_send.at[m, h], ag_recv.at[m, h], dev)

    def reduce_scatter_rest(first_half_terms):
        for h in range(2):
            rs_copy(3, h).wait_recv()
            ybuf[0, 1, h, 1] = ybuf[0, 1, h, 1] + r1[1, 0, h]
            rs_copy(2, h).start()
            rs_copy(0, h).wait_recv()
            ybuf[0, 2, h, 0] = ybuf[0, 2, h, 0] + r1[0, 0, h]
            rs_copy(5, h).start()
        for h in range(2):
            rs_copy(1, h).wait_recv()
            rs_copy(4, h).wait_recv()
            rs_copy(2, h).wait_recv()
            rs_copy(5, h).wait_recv()
            for ab in range(2):
                total = ybuf[0, 3, h, ab] + r1[ab, 1, h] + r2[ab, h]
                xg[me, h, ab] = (first_half_terms(h, ab) + total).astype(BF16).astype(F32)
            for m in range(3):
                ag_copy(m, h).start()

    def wait_rs_sends():
        for e in range(4):
            d2d(e).wait_send()
        for m in range(6):
            for h in range(2):
                rs_copy(m, h).wait_send()

    def wait_ag_sends():
        for m in range(9):
            for h in range(2):
                ag_copy(m, h).wait_send()

    def got(m, h):
        ag_copy(m, h).wait_recv()

    def forward_first(h):
        got(0, h)
        got(1, h)
        for m in (3, 4, 5, 6):
            ag_copy(m, h).start()

    def forward_second(h):
        got(3, h)
        ag_copy(7, h).start()
        got(4, h)
        ag_copy(8, h).start()

    attn = attn_ref[...]
    for t in range(8):
        dc, e = order_cols[t]
        wo_copy(t).wait()
        store_block(dc, e, jnp.dot(attn, wo_buf[t % WO_SLOTS], preferred_element_type=F32))
        if t + WO_SLOTS < 8:
            wo_copy(t + WO_SLOTS).start()
        elif t - WO_SLOTS < GU_SLOTS:
            for copy in gu_copies(t - WO_SLOTS):
                copy.start()
        if t == 0:
            pl.semaphore_wait(barrier, 7)
        if dc == 1:
            d2d(e).start()
        elif e >= 1:
            add_partner(e - 1)
    for k in range(8 - WO_SLOTS, GU_SLOTS):
        for copy in gu_copies(k):
            copy.start()
    for t in range(WD_SLOTS):
        wd_copy(t).start()
    add_partner(3)
    resid_copy.wait()
    reduce_scatter_rest(lambda h, ab: resid_buf[h * half:(h + 1) * half, ab * piece:(ab + 1) * piece].astype(F32))

    parts = []
    for h in range(2):
        sq = jnp.zeros((half, 1), F32)
        for ab in range(2):
            vals = xg[me, h, ab]
            sq = sq + jnp.sum(vals * vals, axis=-1, keepdims=True)
        parts.append(sq)
    sq = jnp.concatenate(parts, axis=0)
    stat_out[...] = jnp.transpose(jnp.broadcast_to(sq, (rows, 128)))[:8]

    def st_copy(j):
        return remote(stat_out, stat.at[j], st_send.at[j], st_recv.at[j], (tp + j) % 8)

    for j in range(1, 8):
        st_copy(j).start()
    sq_all = stat_out[...]
    for j in range(1, 8):
        st_copy(j).wait_recv()
        sq_all = sq_all + stat[j]
    scale = lax.rsqrt(sq_all * (1.0 / width) + EPS)
    rbuf[...] = jnp.transpose(jnp.broadcast_to(scale[:1], (128, rows)))

    def gate_up(k):
        o = owner(*GATHER_ORDER[k])
        for h in range(2):
            r_half = rbuf[h * half:(h + 1) * half, :1]
            for ab in range(2):
                gain = gbuf[o, :, ab * piece:(ab + 1) * piece]
                hbuf[h * half:(h + 1) * half, ab * piece:(ab + 1) * piece] = (
                    xg[o, h, ab] * r_half * gain).astype(BF16)
        s = k % GU_SLOTS
        for copy in gu_copies(k):
            copy.wait()
        normed = hbuf[...]
        gate = jnp.dot(normed, wg_buf[s], preferred_element_type=F32)
        up = jnp.dot(normed, wu_buf[s], preferred_element_type=F32)
        if k == 0:
            acc_g[...] = gate
            acc_u[...] = up
        else:
            acc_g[...] += gate
            acc_u[...] += up
        if k + GU_SLOTS < 8:
            for copy in gu_copies(k + GU_SLOTS):
                copy.start()

    gate_up(0)
    got(2, 0)
    got(2, 1)
    gate_up(1)
    forward_first(0)
    forward_first(1)
    gate_up(2)
    gate_up(3)
    for h in range(2):
        got(5, h)
        got(6, h)
    gate_up(4)
    forward_second(0)
    gate_up(5)
    forward_second(1)
    gate_up(6)
    for h in range(2):
        got(7, h)
        got(8, h)
    gate_up(7)

    gate = acc_g[...].astype(BF16).astype(F32)
    up = acc_u[...].astype(BF16).astype(F32)
    abuf[...] = (jax.nn.silu(gate) * up).astype(BF16)

    wait_rs_sends()
    wait_ag_sends()
    for t in range(8):
        dc, e = order_cols[t]
        wd_copy(t).wait()
        store_block(dc, e, jnp.dot(abuf[...], wd_buf[t % WD_SLOTS], preferred_element_type=F32))
        if t + WD_SLOTS < 8:
            wd_copy(t + WD_SLOTS).start()
        if dc == 1:
            d2d(e).start()
        elif e >= 1:
            add_partner(e - 1)
    add_partner(3)
    reduce_scatter_rest(lambda h, ab: xg[me, h, ab])

    def out_copy(k):
        o = owner(*GATHER_ORDER[k])
        return pltpu.make_async_copy(obuf.at[k], out_hbm.at[:, cols(o)], out_sem.at[k])

    def write_out(k):
        o = owner(*GATHER_ORDER[k])
        for h in range(2):
            for ab in range(2):
                obuf[k, h * half:(h + 1) * half, ab * piece:(ab + 1) * piece] = xg[o, h, ab].astype(BF16)
        out_copy(k).start()

    write_out(0)
    got(2, 0)
    got(2, 1)
    write_out(1)
    forward_first(0)
    forward_first(1)
    write_out(2)
    write_out(3)
    forward_second(0)
    for h in range(2):
        got(5, h)
        got(6, h)
    write_out(4)
    write_out(5)
    forward_second(1)
    write_out(6)
    for h in range(2):
        got(7, h)
        got(8, h)
    write_out(7)
    for j in range(1, 8):
        st_copy(j).wait_send()
    wait_rs_sends()
    wait_ag_sends()
    for k in range(8):
        out_copy(k).wait()


def mlp_tail(attn_out, resid_in, gain_mlp, w_out, w_gate, w_up, w_down):
    rows, width = resid_in.shape
    depth = w_out.shape[0]
    ffn = w_gate.shape[1]
    block = width // 8
    piece = block // 2
    half = rows // 2
    dma = pltpu.SemaphoreType.DMA
    return pl.pallas_call(
        tail_kernel,
        out_shape=jax.ShapeDtypeStruct((rows, width), BF16),
        in_specs=[pl.BlockSpec(memory_space=pltpu.VMEM)] * 2 + [pl.BlockSpec(memory_space=pl.ANY)] * 5,
        out_specs=pl.BlockSpec(memory_space=pl.ANY),
        scratch_shapes=[
            pltpu.VMEM((WO_SLOTS, depth, block), BF16),
            pltpu.VMEM((GU_SLOTS, block, ffn), BF16),
            pltpu.VMEM((GU_SLOTS, block, ffn), BF16),
            pltpu.VMEM((WD_SLOTS, ffn, block), BF16),
            pltpu.VMEM((2, 4, 2, 2, half, piece), F32),
            pltpu.VMEM((4, 2, 2, half, piece), F32),
            pltpu.VMEM((2, 2, 2, half, piece), F32),
            pltpu.VMEM((2, 2, half, piece), F32),
            pltpu.VMEM((8, 2, 2, half, piece), F32),
            pltpu.VMEM((rows, ffn), F32),
            pltpu.VMEM((rows, ffn), F32),
            pltpu.VMEM((rows, ffn), BF16),
            pltpu.VMEM((rows, block), BF16),
            pltpu.VMEM((rows, block), BF16),
            pltpu.VMEM((8, rows, block), BF16),
            pltpu.VMEM((8, 8, rows), F32),
            pltpu.VMEM((8, rows), F32),
            pltpu.VMEM((8, 1, block), F32),
            pltpu.VMEM((rows, 128), F32),
            dma((WO_SLOTS,)),
            dma((2, GU_SLOTS)),
            dma((WD_SLOTS,)),
            dma(()),
            dma((8,)),
            dma((4,)),
            dma((4,)),
            dma((6, 2)),
            dma((6, 2)),
            dma((9, 2)),
            dma((9, 2)),
            dma((8,)),
            dma((8,)),
        ],
        compiler_params=pltpu.CompilerParams(collective_id=0, has_side_effects=True,
                                             vmem_limit_bytes=67_000_000),
    )(attn_out, gain_mlp.reshape(1, width), resid_in, w_out, w_gate, w_up, w_down)


def solution(mesh):
    def layer_local(resid_in, positions, k_cache, v_cache, gain_attn, w_query, w_key, w_value,
                    w_out, gain_mlp, w_gate, w_up, w_down):
        attn_out, k_full, v_full = attention_block(resid_in, positions, k_cache, v_cache,
                                                   gain_attn, w_query, w_key, w_value)
        resid_out = mlp_tail(attn_out, resid_in, gain_mlp, w_out, w_gate, w_up, w_down)
        return resid_out, k_full, v_full

    row_spec = P('dp', None)
    cache_spec = P('dp', None, 'tp', None)
    col_spec = P(None, 'tp')
    split_rows = P('tp', None)
    return jax.shard_map(layer_local, mesh=mesh,
                         in_specs=(row_spec, P('dp'), cache_spec, cache_spec, P(), col_spec, col_spec,
                                   col_spec, split_rows, P(), col_spec, col_spec, split_rows),
                         out_specs=(row_spec, cache_spec, cache_spec), check_vma=False)
```

```python
import math
import jax
import jax.numpy as jnp
from jax import lax
from jax.experimental import pallas as pl
from jax.experimental.pallas import tpu as pltpu
from jax.sharding import PartitionSpec as P

EPS = 1e-5
ROPE_THETA = 500000.0
ROPE_FACTOR = 8.0
LOW_FACTOR = 1.0
HIGH_FACTOR = 4.0
ORIG_CTX = 8192.0


F32 = jnp.float32
BF16 = jnp.bfloat16
BLOCK_SEQS = 32
N_CHUNKS = 6


def inverse_frequencies(head_dim):
    half_dim = head_dim // 2
    exponents = jnp.arange(half_dim, dtype=jnp.float32) * (2.0 / head_dim)
    inv_freq = 1.0 / jnp.power(ROPE_THETA, exponents)
    wavelen = (2.0 * math.pi) / inv_freq
    smooth = (ORIG_CTX / wavelen - LOW_FACTOR) / (HIGH_FACTOR - LOW_FACTOR)
    blended = (1.0 - smooth) * inv_freq / ROPE_FACTOR + smooth * inv_freq
    inv_freq = jnp.where(wavelen < ORIG_CTX / HIGH_FACTOR, inv_freq,
                         jnp.where(wavelen > ORIG_CTX / LOW_FACTOR, inv_freq / ROPE_FACTOR, blended))
    return jnp.concatenate([inv_freq, inv_freq]).reshape(1, head_dim)


def attention_kernel(pos_ref, pos_row_ref, inv_ref, gain_ref, resid_hbm, wq_hbm, wk_hbm, wv_hbm, kc_hbm, vc_hbm,
                     out_ref, ko_hbm, vo_hbm,
                     resid_buf, hbuf, gbuf, wbuf, kbuf, vbuf, acc, qbuf, knew, vnew, obuf,
                     resid_sem, w_sem, in_sem, back_sem):
    rows, width = hbuf.shape
    q_width = wq_hbm.shape[1]
    head_dim = kbuf.shape[2]
    slots = kbuf.shape[1]
    heads = q_width // head_dim
    chunk = width // N_CHUNKS
    tiles = width // 128
    n_blocks = rows // BLOCK_SEQS

    resid_copy = pltpu.make_async_copy(resid_hbm, resid_buf, resid_sem)
    resid_copy.start()

    def w_copies(i):
        r = pl.ds(i * chunk, chunk)
        return (pltpu.make_async_copy(wq_hbm.at[r], wbuf.at[i, :, pl.ds(0, q_width)], w_sem.at[i, 0]),
                pltpu.make_async_copy(wk_hbm.at[r], wbuf.at[i, :, pl.ds(q_width, head_dim)], w_sem.at[i, 1]),
                pltpu.make_async_copy(wv_hbm.at[r], wbuf.at[i, :, pl.ds(q_width + head_dim, head_dim)],
                                      w_sem.at[i, 2]))

    def cache_in(blk):
        r = pl.ds(blk * BLOCK_SEQS, BLOCK_SEQS)
        return (pltpu.make_async_copy(kc_hbm.at[r], kbuf.at[r], in_sem.at[0, blk]),
                pltpu.make_async_copy(vc_hbm.at[r], vbuf.at[r], in_sem.at[1, blk]))

    def cache_back(blk):
        r = pl.ds(blk * BLOCK_SEQS, BLOCK_SEQS)
        return (pltpu.make_async_copy(kbuf.at[r], ko_hbm.at[r], back_sem.at[0, blk]),
                pltpu.make_async_copy(vbuf.at[r], vo_hbm.at[r], back_sem.at[1, blk]))

    for i in range(N_CHUNKS):
        for copy in w_copies(i):
            copy.start()

    pos_rows = jnp.transpose(jnp.broadcast_to(pos_row_ref[...].astype(F32), (head_dim, rows)))
    angles = pos_rows * inv_ref[...]
    cos_t = jnp.cos(angles)
    sin_t = jnp.sin(angles)
    lanes = lax.broadcasted_iota(jnp.int32, (rows, head_dim), 1)
    sin_t = jnp.where(lanes < head_dim // 2, -sin_t, sin_t)

    def rope(v):
        v = v.astype(BF16).astype(F32)
        return (v * cos_t + pltpu.roll(v, head_dim // 2, 1) * sin_t).astype(BF16).astype(F32)

    gbuf[...] = gain_ref[...].astype(F32)
    qbuf[...] = jnp.zeros_like(qbuf)

    resid_copy.wait()
    sq = jnp.zeros((rows, 128), F32)
    for j in range(tiles):
        vals = resid_buf[:, j * 128:(j + 1) * 128].astype(F32)
        sq = sq + vals * vals
    scale = lax.rsqrt(jnp.sum(sq, axis=-1, keepdims=True) * (1.0 / width) + EPS)
    scale = jnp.broadcast_to(scale, (rows, 128))
    for j in range(tiles):
        vals = resid_buf[:, j * 128:(j + 1) * 128].astype(F32)
        hbuf[:, j * 128:(j + 1) * 128] = (vals * scale * gbuf[j:j + 1, :]).astype(BF16)

    for i in range(N_CHUNKS):
        for copy in w_copies(i):
            copy.wait()
        if 1 <= i <= n_blocks:
            for copy in cache_in(i - 1):
                copy.start()
        part = jnp.dot(hbuf[:, i * chunk:(i + 1) * chunk], wbuf[i], preferred_element_type=F32)
        if i == 0:
            acc[...] = part
        else:
            acc[...] += part
    for h in range(heads):
        qbuf[:, h, :] = rope(acc[:, h * head_dim:(h + 1) * head_dim])
    knew[...] = rope(acc[:, q_width:q_width + head_dim])
    vnew[...] = acc[:, q_width + head_dim:q_width + 2 * head_dim].astype(BF16).astype(F32)

    sub_iota = lax.broadcasted_iota(jnp.int32, (16, head_dim), 0)
    lane_iota = lax.broadcasted_iota(jnp.int32, (8, slots), 1)
    inv_sqrt = 1.0 / math.sqrt(head_dim)

    def block_step(blk, carry):
        first = blk * BLOCK_SEQS
        for copy in cache_in(blk):
            copy.wait()
        pos = [pos_ref[first + j] for j in range(BLOCK_SEQS)]
        for buf, new in ((kbuf, knew), (vbuf, vnew)):
            for j0 in range(0, BLOCK_SEQS, 16):
                merged = []
                for j in range(j0, j0 + 16):
                    base = pl.multiple_of((pos[j] // 16) * 16, 16)
                    old = buf[first + j, pl.ds(base, 16), :].astype(F32)
                    row = jnp.broadcast_to(new[pl.ds(first + j, 1), :], (16, head_dim))
                    merged.append((base, jnp.where(sub_iota == pos[j] - base, row, old).astype(BF16)))
                for j in range(j0, j0 + 16):
                    base, tile = merged[j - j0]
                    buf[first + j, pl.ds(base, 16), :] = tile
        probs = []
        for j in range(0, BLOCK_SEQS, 2):
            q2 = qbuf[pl.ds(first + j, 2)].reshape(16, head_dim).astype(BF16)
            k2 = kbuf[pl.ds(first + j, 2)].reshape(2 * slots, head_dim)
            scores = lax.dot_general(q2, k2, (((1,), (1,)), ((), ())), preferred_element_type=F32)
            pair = []
            for i in range(2):
                s_one = scores[8 * i:8 * (i + 1), slots * i:slots * (i + 1)] * inv_sqrt
                s_one = jnp.where(lane_iota <= pos[j + i], s_one, -jnp.inf)
                s_one = jnp.exp(s_one - jnp.max(s_one, axis=-1, keepdims=True))
                pair.append(s_one / jnp.sum(s_one, axis=-1, keepdims=True))
            probs.append(jnp.concatenate(pair, axis=0).astype(BF16))
        for j in range(0, BLOCK_SEQS, 2):
            v2 = jnp.concatenate([vbuf[first + j], vbuf[first + j + 1]], axis=1)
            both = jnp.dot(probs[j // 2], v2, preferred_element_type=F32)
            for i in range(2):
                obuf[first + j + i] = both[8 * i:8 * (i + 1), head_dim * i:head_dim * (i + 1)]
        for copy in cache_back(blk):
            copy.start()
        return carry

    lax.fori_loop(0, n_blocks, block_step, 0)
    for h in range(heads):
        out_ref[:, h * head_dim:(h + 1) * head_dim] = obuf[:, h, :].astype(BF16)
    for blk in range(n_blocks):
        for copy in cache_back(blk):
            copy.wait()


def attention(resid_in, positions, k_cache, v_cache, gain_attn, w_query, w_key, w_value):
    rows, width = resid_in.shape
    slots, head_dim = k_cache.shape[1], k_cache.shape[3]
    q_width = w_query.shape[1]
    qkv = q_width + 2 * head_dim
    n_blocks = rows // BLOCK_SEQS
    dma = pltpu.SemaphoreType.DMA
    flat = (rows, slots, head_dim)
    vmem = pl.BlockSpec(memory_space=pltpu.VMEM)
    anywhere = pl.BlockSpec(memory_space=pl.ANY)
    attn_out, k_full, v_full = pl.pallas_call(
        attention_kernel,
        out_shape=(jax.ShapeDtypeStruct((rows, q_width), BF16),
                   jax.ShapeDtypeStruct(flat, BF16), jax.ShapeDtypeStruct(flat, BF16)),
        in_specs=[pl.BlockSpec(memory_space=pltpu.SMEM), vmem, vmem, vmem] + [anywhere] * 6,
        out_specs=(vmem, anywhere, anywhere),
        scratch_shapes=[
            pltpu.VMEM((rows, width), BF16),
            pltpu.VMEM((rows, width), BF16),
            pltpu.VMEM((width // 128, 128), F32),
            pltpu.VMEM((N_CHUNKS, width // N_CHUNKS, qkv), BF16),
            pltpu.VMEM(flat, BF16),
            pltpu.VMEM(flat, BF16),
            pltpu.VMEM((rows, qkv), F32),
            pltpu.VMEM((rows, 8, head_dim), F32),
            pltpu.VMEM((rows, head_dim), F32),
            pltpu.VMEM((rows, head_dim), F32),
            pltpu.VMEM((rows, 8, head_dim), F32),
            dma(()),
            dma((N_CHUNKS, 3)),
            dma((2, n_blocks)),
            dma((2, n_blocks)),
        ],
        compiler_params=pltpu.CompilerParams(vmem_limit_bytes=60_000_000),
    )(positions, positions.reshape(1, rows), inverse_frequencies(head_dim), gain_attn.reshape(width // 128, 128),
      resid_in, w_query, w_key, w_value, k_cache.reshape(flat), v_cache.reshape(flat))
    return attn_out, k_full.reshape(k_cache.shape), v_full.reshape(v_cache.shape)


REL = ((1, 1), (0, 1), (1, 0), (0, 0))
WO_SLOTS = 4
GU_SLOTS = 5
WD_SLOTS = 4
GATHER_ORDER = ((0, 3), (1, 3), (0, 1), (0, 2), (1, 1), (1, 2), (0, 0), (1, 0))


def flip(coord, do_flip):
    return 1 - coord if do_flip else coord


def tail_kernel(attn_ref, gain_ref, resid_hbm, wo_hbm, wg_hbm, wu_hbm, wd_hbm, out_hbm,
                wo_buf, wg_buf, wu_buf, wd_buf, ybuf, dbuf, r1, r2, xg, acc_g, acc_u, abuf, hbuf,
                resid_buf, obuf, stat, stat_out, gbuf, rbuf,
                wo_sem, gu_sem, wd_sem, resid_sem, out_sem, d_send, d_recv, rs_send, rs_recv,
                ag_send, ag_recv, st_send, st_recv):
    rows = attn_ref.shape[0]
    half = rows // 2
    block = wo_buf.shape[2]
    piece = block // 2
    width = 8 * block

    tp = lax.axis_index('tp')
    core = tp % 2
    x_pos = (tp // 2) % 2
    y_pos = tp // 4

    def device(flip_core, rel):
        flip_y, flip_x = rel
        return flip(y_pos, flip_y) * 4 + flip(x_pos, flip_x) * 2 + flip(core, flip_core)

    def owner(flip_core, e):
        return device(flip_core, REL[e])

    def cols(o):
        return pl.ds(pl.multiple_of(o * block, block), block)

    me = owner(0, 3)
    dev_d = owner(1, 3)
    dev_x = owner(0, 1)
    dev_y = owner(0, 2)

    def remote(src, dst, send, recv, dev):
        return pltpu.make_async_remote_copy(src_ref=src, dst_ref=dst, send_sem=send, recv_sem=recv,
                                            device_id={'tp': dev}, device_id_type=pl.DeviceIdType.MESH)

    order_cols = [(1 - t % 2, t // 2) for t in range(8)]

    def wo_copy(t):
        o = owner(*order_cols[t])
        return pltpu.make_async_copy(wo_hbm.at[:, cols(o)], wo_buf.at[t % WO_SLOTS], wo_sem.at[t % WO_SLOTS])

    def gu_copies(k):
        o = owner(*GATHER_ORDER[k])
        s = k % GU_SLOTS
        return (pltpu.make_async_copy(wg_hbm.at[cols(o), :], wg_buf.at[s], gu_sem.at[0, s]),
                pltpu.make_async_copy(wu_hbm.at[cols(o), :], wu_buf.at[s], gu_sem.at[1, s]))

    def wd_copy(t):
        o = owner(*order_cols[t])
        return pltpu.make_async_copy(wd_hbm.at[:, cols(o)], wd_buf.at[t % WD_SLOTS], wd_sem.at[t % WD_SLOTS])

    for t in range(WO_SLOTS):
        wo_copy(t).start()
    resid_copy = pltpu.make_async_copy(resid_hbm.at[:, cols(me)], resid_buf, resid_sem)
    resid_copy.start()

    barrier = pltpu.get_barrier_semaphore()
    for j in range(1, 8):
        pl.semaphore_signal(barrier, inc=1, device_id={'tp': (tp + j) % 8}, device_id_type=pl.DeviceIdType.MESH)

    gbuf[...] = gain_ref[...].astype(F32)

    def store_block(dc, e, res):
        for h in range(2):
            for ab in range(2):
                ybuf[dc, e, h, ab] = res[h * half:(h + 1) * half, ab * piece:(ab + 1) * piece]

    def d2d(e):
        return remote(ybuf.at[1, e], dbuf.at[e], d_send.at[e], d_recv.at[e], dev_d)

    def rs_copy(m, h):
        src, dst, dev = (
            (ybuf.at[0, 0, h, 0], r1.at[0, 0, h], dev_x),
            (ybuf.at[0, 1, h, 0], r1.at[0, 1, h], dev_x),
            (ybuf.at[0, 1, h, 1], r2.at[1, h], dev_x),
            (ybuf.at[0, 0, h, 1], r1.at[1, 0, h], dev_y),
            (ybuf.at[0, 2, h, 1], r1.at[1, 1, h], dev_y),
            (ybuf.at[0, 2, h, 0], r2.at[0, h], dev_y),
        )[m]
        return remote(src, dst, rs_send.at[m, h], rs_recv.at[m, h], dev)

    def add_partner(e):
        d2d(e).wait_recv()
        for h in range(2):
            for ab in range(2):
                ybuf[0, e, h, ab] = ybuf[0, e, h, ab] + dbuf[e, h, ab]
            if e == 0:
                rs_copy(0, h).start()
                rs_copy(3, h).start()
            if e == 1:
                rs_copy(1, h).start()
            if e == 2:
                rs_copy(4, h).start()

    def ag_copy(m, h):
        ox, oy, oxy = owner(0, 1), owner(0, 2), owner(0, 0)
        ref, dev = (
            (xg.at[me, h], dev_x),
            (xg.at[me, h], dev_y),
            (xg.at[me, h], dev_d),
            (xg.at[oy, h, 0], dev_x),
            (xg.at[ox, h, 1], dev_y),
            (xg.at[ox, h], dev_d),
            (xg.at[oy, h], dev_d),
            (xg.at[oxy, h, 0], dev_d),
            (xg.at[oxy, h, 1], dev_d),
        )[m]
        return remote(ref, ref, ag_send.at[m, h], ag_recv.at[m, h], dev)

    def reduce_scatter_rest(first_half_terms):
        for h in range(2):
            rs_copy(3, h).wait_recv()
            ybuf[0, 1, h, 1] = ybuf[0, 1, h, 1] + r1[1, 0, h]
            rs_copy(2, h).start()
            rs_copy(0, h).wait_recv()
            ybuf[0, 2, h, 0] = ybuf[0, 2, h, 0] + r1[0, 0, h]
            rs_copy(5, h).start()
        for h in range(2):
            rs_copy(1, h).wait_recv()
            rs_copy(4, h).wait_recv()
            rs_copy(2, h).wait_recv()
            rs_copy(5, h).wait_recv()
            for ab in range(2):
                total = ybuf[0, 3, h, ab] + r1[ab, 1, h] + r2[ab, h]
                xg[me, h, ab] = (first_half_terms(h, ab) + total).astype(BF16).astype(F32)
            for m in range(3):
                ag_copy(m, h).start()

    def wait_rs_sends():
        for e in range(4):
            d2d(e).wait_send()
        for m in range(6):
            for h in range(2):
                rs_copy(m, h).wait_send()

    def wait_ag_sends():
        for m in range(9):
            for h in range(2):
                ag_copy(m, h).wait_send()

    def got(m, h):
        ag_copy(m, h).wait_recv()

    def forward_first(h):
        got(0, h)
        got(1, h)
        for m in (3, 4, 5, 6):
            ag_copy(m, h).start()

    def forward_second(h):
        got(3, h)
        ag_copy(7, h).start()
        got(4, h)
        ag_copy(8, h).start()

    attn = attn_ref[...]
    for t in range(8):
        dc, e = order_cols[t]
        wo_copy(t).wait()
        store_block(dc, e, jnp.dot(attn, wo_buf[t % WO_SLOTS], preferred_element_type=F32))
        if t + WO_SLOTS < 8:
            wo_copy(t + WO_SLOTS).start()
        elif t - WO_SLOTS < GU_SLOTS:
            for copy in gu_copies(t - WO_SLOTS):
                copy.start()
        if t == 0:
            pl.semaphore_wait(barrier, 7)
        if dc == 1:
            d2d(e).start()
        elif e >= 1:
            add_partner(e - 1)
    for k in range(8 - WO_SLOTS, GU_SLOTS):
        for copy in gu_copies(k):
            copy.start()
    for t in range(WD_SLOTS):
        wd_copy(t).start()
    add_partner(3)
    resid_copy.wait()
    reduce_scatter_rest(lambda h, ab: resid_buf[h * half:(h + 1) * half, ab * piece:(ab + 1) * piece].astype(F32))

    parts = []
    for h in range(2):
        sq = jnp.zeros((half, 1), F32)
        for ab in range(2):
            vals = xg[me, h, ab]
            sq = sq + jnp.sum(vals * vals, axis=-1, keepdims=True)
        parts.append(sq)
    sq = jnp.concatenate(parts, axis=0)
    stat_out[...] = jnp.transpose(jnp.broadcast_to(sq, (rows, 128)))[:8]

    def st_copy(j):
        return remote(stat_out, stat.at[j], st_send.at[j], st_recv.at[j], (tp + j) % 8)

    for j in range(1, 8):
        st_copy(j).start()
    sq_all = stat_out[...]
    for j in range(1, 8):
        st_copy(j).wait_recv()
        sq_all = sq_all + stat[j]
    scale = lax.rsqrt(sq_all * (1.0 / width) + EPS)
    rbuf[...] = jnp.transpose(jnp.broadcast_to(scale[:1], (128, rows)))

    def gate_up(k):
        o = owner(*GATHER_ORDER[k])
        for h in range(2):
            r_half = rbuf[h * half:(h + 1) * half, :]
            for ab in range(2):
                for j in range(piece // 128):
                    gain = gbuf[pl.ds(o * (block // 128) + ab * (piece // 128) + j, 1), :]
                    hbuf[h * half:(h + 1) * half, ab * piece + j * 128:ab * piece + (j + 1) * 128] = (
                        xg[o, h, ab, :, j * 128:(j + 1) * 128] * r_half * gain).astype(BF16)
        s = k % GU_SLOTS
        for copy in gu_copies(k):
            copy.wait()
        normed = hbuf[...]
        gate = jnp.dot(normed, wg_buf[s], preferred_element_type=F32)
        up = jnp.dot(normed, wu_buf[s], preferred_element_type=F32)
        if k == 0:
            acc_g[...] = gate
            acc_u[...] = up
        else:
            acc_g[...] += gate
            acc_u[...] += up
        if k + GU_SLOTS < 8:
            for copy in gu_copies(k + GU_SLOTS):
                copy.start()

    gate_up(0)
    got(2, 0)
    got(2, 1)
    gate_up(1)
    forward_first(0)
    forward_first(1)
    gate_up(2)
    gate_up(3)
    for h in range(2):
        got(5, h)
        got(6, h)
    gate_up(4)
    forward_second(0)
    gate_up(5)
    forward_second(1)
    gate_up(6)
    for h in range(2):
        got(7, h)
        got(8, h)
    gate_up(7)

    gate = acc_g[...].astype(BF16).astype(F32)
    up = acc_u[...].astype(BF16).astype(F32)
    abuf[...] = (jax.nn.silu(gate) * up).astype(BF16)

    wait_rs_sends()
    wait_ag_sends()
    for t in range(8):
        dc, e = order_cols[t]
        wd_copy(t).wait()
        store_block(dc, e, jnp.dot(abuf[...], wd_buf[t % WD_SLOTS], preferred_element_type=F32))
        if t + WD_SLOTS < 8:
            wd_copy(t + WD_SLOTS).start()
        if dc == 1:
            d2d(e).start()
        elif e >= 1:
            add_partner(e - 1)
    add_partner(3)
    reduce_scatter_rest(lambda h, ab: xg[me, h, ab])

    def out_copy(k):
        o = owner(*GATHER_ORDER[k])
        return pltpu.make_async_copy(obuf.at[k], out_hbm.at[:, cols(o)], out_sem.at[k])

    def write_out(k):
        o = owner(*GATHER_ORDER[k])
        for h in range(2):
            for ab in range(2):
                obuf[k, h * half:(h + 1) * half, ab * piece:(ab + 1) * piece] = xg[o, h, ab].astype(BF16)
        out_copy(k).start()

    write_out(0)
    got(2, 0)
    got(2, 1)
    write_out(1)
    forward_first(0)
    forward_first(1)
    write_out(2)
    write_out(3)
    forward_second(0)
    for h in range(2):
        got(5, h)
        got(6, h)
    write_out(4)
    write_out(5)
    forward_second(1)
    write_out(6)
    for h in range(2):
        got(7, h)
        got(8, h)
    write_out(7)
    for j in range(1, 8):
        st_copy(j).wait_send()
    wait_rs_sends()
    wait_ag_sends()
    for k in range(8):
        out_copy(k).wait()


def mlp_tail(attn_out, resid_in, gain_mlp, w_out, w_gate, w_up, w_down):
    rows, width = resid_in.shape
    depth = w_out.shape[0]
    ffn = w_gate.shape[1]
    block = width // 8
    piece = block // 2
    half = rows // 2
    dma = pltpu.SemaphoreType.DMA
    return pl.pallas_call(
        tail_kernel,
        out_shape=jax.ShapeDtypeStruct((rows, width), BF16),
        in_specs=[pl.BlockSpec(memory_space=pltpu.VMEM)] * 2 + [pl.BlockSpec(memory_space=pl.ANY)] * 5,
        out_specs=pl.BlockSpec(memory_space=pl.ANY),
        scratch_shapes=[
            pltpu.VMEM((WO_SLOTS, depth, block), BF16),
            pltpu.VMEM((GU_SLOTS, block, ffn), BF16),
            pltpu.VMEM((GU_SLOTS, block, ffn), BF16),
            pltpu.VMEM((WD_SLOTS, ffn, block), BF16),
            pltpu.VMEM((2, 4, 2, 2, half, piece), F32),
            pltpu.VMEM((4, 2, 2, half, piece), F32),
            pltpu.VMEM((2, 2, 2, half, piece), F32),
            pltpu.VMEM((2, 2, half, piece), F32),
            pltpu.VMEM((8, 2, 2, half, piece), F32),
            pltpu.VMEM((rows, ffn), F32),
            pltpu.VMEM((rows, ffn), F32),
            pltpu.VMEM((rows, ffn), BF16),
            pltpu.VMEM((rows, block), BF16),
            pltpu.VMEM((rows, block), BF16),
            pltpu.VMEM((8, rows, block), BF16),
            pltpu.VMEM((8, 8, rows), F32),
            pltpu.VMEM((8, rows), F32),
            pltpu.VMEM((width // 128, 128), F32),
            pltpu.VMEM((rows, 128), F32),
            dma((WO_SLOTS,)),
            dma((2, GU_SLOTS)),
            dma((WD_SLOTS,)),
            dma(()),
            dma((8,)),
            dma((4,)),
            dma((4,)),
            dma((6, 2)),
            dma((6, 2)),
            dma((9, 2)),
            dma((9, 2)),
            dma((8,)),
            dma((8,)),
        ],
        compiler_params=pltpu.CompilerParams(collective_id=0, has_side_effects=True,
                                             vmem_limit_bytes=67_000_000),
    )(attn_out, gain_mlp.reshape(width // 128, 128), resid_in, w_out, w_gate, w_up, w_down)


def solution(mesh):
    def layer_local(resid_in, positions, k_cache, v_cache, gain_attn, w_query, w_key, w_value,
                    w_out, gain_mlp, w_gate, w_up, w_down):
        attn_out, k_full, v_full = attention(resid_in, positions, k_cache, v_cache, gain_attn,
                                             w_query, w_key, w_value)
        resid_out = mlp_tail(attn_out, resid_in, gain_mlp, w_out, w_gate, w_up, w_down)
        return resid_out, k_full, v_full

    row_spec = P('dp', None)
    cache_spec = P('dp', None, 'tp', None)
    col_spec = P(None, 'tp')
    split_rows = P('tp', None)
    return jax.shard_map(layer_local, mesh=mesh,
                         in_specs=(row_spec, P('dp'), cache_spec, cache_spec, P(), col_spec, col_spec,
                                   col_spec, split_rows, P(), col_spec, col_spec, split_rows),
                         out_specs=(row_spec, cache_spec, cache_spec), check_vma=False)
```

```python
import math
import jax
import numpy as np
import jax.numpy as jnp
from jax import lax
from jax.experimental import pallas as pl
from jax.experimental.pallas import tpu as pltpu
from jax.sharding import PartitionSpec as P

EPS = 1e-5
ROPE_THETA = 500000.0
ROPE_FACTOR = 8.0
LOW_FACTOR = 1.0
HIGH_FACTOR = 4.0
ORIG_CTX = 8192.0


F32 = jnp.float32
BF16 = jnp.bfloat16
BLOCK_SEQS = 32
N_CHUNKS = 6


def in_hbm(x):
    return pltpu.with_memory_space_constraint(x, pltpu.HBM)


def in_vmem(x):
    return pltpu.with_memory_space_constraint(x, pltpu.VMEM)


def inverse_frequencies(head_dim):
    exponents = np.arange(head_dim // 2, dtype=np.float32) * np.float32(2.0 / head_dim)
    inv_freq = (np.float32(1.0) / np.power(np.float32(ROPE_THETA), exponents)).astype(np.float32)
    wavelen = np.float32(2.0 * math.pi) / inv_freq
    smooth = (np.float32(ORIG_CTX) / wavelen - np.float32(LOW_FACTOR)) / np.float32(HIGH_FACTOR - LOW_FACTOR)
    blended = (np.float32(1.0) - smooth) * inv_freq / np.float32(ROPE_FACTOR) + smooth * inv_freq
    inv_freq = np.where(wavelen < ORIG_CTX / HIGH_FACTOR, inv_freq,
                        np.where(wavelen > ORIG_CTX / LOW_FACTOR, inv_freq / np.float32(ROPE_FACTOR), blended))
    return jnp.asarray(np.concatenate([inv_freq, inv_freq]).astype(np.float32).reshape(1, head_dim))


def attention_kernel(pos_hbm, pos_row_hbm, inv_hbm, gain_hbm, resid_hbm, wq_hbm, wk_hbm, wv_hbm, kc_hbm, vc_hbm,
                     out_ref, ko_hbm, vo_hbm,
                     pos_ref, pos_row_ref, inv_ref, gain_ref,
                     resid_buf, hbuf, gbuf, wbuf, kbuf, vbuf, acc, qbuf, knew, vnew, obuf,
                     small_sem, resid_sem, w_sem, in_sem, back_sem):
    rows, width = hbuf.shape
    q_width = wq_hbm.shape[1]
    head_dim = kbuf.shape[2]
    slots = kbuf.shape[1]
    heads = q_width // head_dim
    chunk = width // N_CHUNKS
    tiles = width // 128
    n_blocks = rows // BLOCK_SEQS

    resid_copy = pltpu.make_async_copy(resid_hbm, resid_buf, resid_sem)
    resid_copy.start()
    small_copies = [pltpu.make_async_copy(src, dst, small_sem.at[i]) for i, (src, dst) in enumerate((
        (pos_row_hbm, pos_row_ref), (inv_hbm, inv_ref), (gain_hbm, gain_ref), (pos_hbm, pos_ref)))]
    for copy in small_copies:
        copy.start()

    def w_copies(i):
        r = pl.ds(i * chunk, chunk)
        return (pltpu.make_async_copy(wq_hbm.at[r], wbuf.at[i, :, pl.ds(0, q_width)], w_sem.at[i, 0]),
                pltpu.make_async_copy(wk_hbm.at[r], wbuf.at[i, :, pl.ds(q_width, head_dim)], w_sem.at[i, 1]),
                pltpu.make_async_copy(wv_hbm.at[r], wbuf.at[i, :, pl.ds(q_width + head_dim, head_dim)],
                                      w_sem.at[i, 2]))

    def cache_in(blk):
        r = pl.ds(blk * BLOCK_SEQS, BLOCK_SEQS)
        return (pltpu.make_async_copy(kc_hbm.at[r], kbuf.at[r], in_sem.at[0, blk]),
                pltpu.make_async_copy(vc_hbm.at[r], vbuf.at[r], in_sem.at[1, blk]))

    def cache_back(blk):
        r = pl.ds(blk * BLOCK_SEQS, BLOCK_SEQS)
        return (pltpu.make_async_copy(kbuf.at[r], ko_hbm.at[r], back_sem.at[0, blk]),
                pltpu.make_async_copy(vbuf.at[r], vo_hbm.at[r], back_sem.at[1, blk]))

    for i in range(N_CHUNKS):
        for copy in w_copies(i):
            copy.start()

    for copy in small_copies:
        copy.wait()
    pos_rows = jnp.transpose(jnp.broadcast_to(pos_row_ref[...].astype(F32), (head_dim, rows)))
    angles = pos_rows * inv_ref[...]
    cos_t = jnp.cos(angles)
    sin_t = jnp.sin(angles)
    lanes = lax.broadcasted_iota(jnp.int32, (rows, head_dim), 1)
    sin_t = jnp.where(lanes < head_dim // 2, -sin_t, sin_t)

    def rope(v):
        v = v.astype(BF16).astype(F32)
        return (v * cos_t + pltpu.roll(v, head_dim // 2, 1) * sin_t).astype(BF16).astype(F32)

    gbuf[...] = gain_ref[...].astype(F32)
    qbuf[...] = jnp.zeros_like(qbuf)

    resid_copy.wait()
    sq = jnp.zeros((rows, 128), F32)
    for j in range(tiles):
        vals = resid_buf[:, j * 128:(j + 1) * 128].astype(F32)
        sq = sq + vals * vals
    scale = lax.rsqrt(jnp.sum(sq, axis=-1, keepdims=True) * (1.0 / width) + EPS)
    scale = jnp.broadcast_to(scale, (rows, 128))
    for j in range(tiles):
        vals = resid_buf[:, j * 128:(j + 1) * 128].astype(F32)
        hbuf[:, j * 128:(j + 1) * 128] = (vals * scale * gbuf[j:j + 1, :]).astype(BF16)

    for i in range(N_CHUNKS):
        for copy in w_copies(i):
            copy.wait()
        if 1 <= i <= n_blocks:
            for copy in cache_in(i - 1):
                copy.start()
        part = jnp.dot(hbuf[:, i * chunk:(i + 1) * chunk], wbuf[i], preferred_element_type=F32)
        if i == 0:
            acc[...] = part
        else:
            acc[...] += part
    for h in range(heads):
        qbuf[:, h, :] = rope(acc[:, h * head_dim:(h + 1) * head_dim])
    knew[...] = rope(acc[:, q_width:q_width + head_dim])
    vnew[...] = acc[:, q_width + head_dim:q_width + 2 * head_dim].astype(BF16).astype(F32)

    sub_iota = lax.broadcasted_iota(jnp.int32, (16, head_dim), 0)
    lane_iota = lax.broadcasted_iota(jnp.int32, (8, slots), 1)
    inv_sqrt = 1.0 / math.sqrt(head_dim)

    def block_step(blk, carry):
        first = blk * BLOCK_SEQS
        for copy in cache_in(blk):
            copy.wait()
        pos = [pos_ref[first + j] for j in range(BLOCK_SEQS)]
        for buf, new in ((kbuf, knew), (vbuf, vnew)):
            for j0 in range(0, BLOCK_SEQS, 16):
                merged = []
                for j in range(j0, j0 + 16):
                    base = pl.multiple_of((pos[j] // 16) * 16, 16)
                    old = buf[first + j, pl.ds(base, 16), :].astype(F32)
                    row = jnp.broadcast_to(new[pl.ds(first + j, 1), :], (16, head_dim))
                    merged.append((base, jnp.where(sub_iota == pos[j] - base, row, old).astype(BF16)))
                for j in range(j0, j0 + 16):
                    base, tile = merged[j - j0]
                    buf[first + j, pl.ds(base, 16), :] = tile
        probs = []
        for j in range(0, BLOCK_SEQS, 2):
            q2 = qbuf[pl.ds(first + j, 2)].reshape(16, head_dim).astype(BF16)
            k2 = kbuf[pl.ds(first + j, 2)].reshape(2 * slots, head_dim)
            scores = lax.dot_general(q2, k2, (((1,), (1,)), ((), ())), preferred_element_type=F32)
            pair = []
            for i in range(2):
                s_one = scores[8 * i:8 * (i + 1), slots * i:slots * (i + 1)] * inv_sqrt
                s_one = jnp.where(lane_iota <= pos[j + i], s_one, -jnp.inf)
                s_one = jnp.exp(s_one - jnp.max(s_one, axis=-1, keepdims=True))
                pair.append(s_one / jnp.sum(s_one, axis=-1, keepdims=True))
            probs.append(jnp.concatenate(pair, axis=0).astype(BF16))
        for j in range(0, BLOCK_SEQS, 2):
            v2 = jnp.concatenate([vbuf[first + j], vbuf[first + j + 1]], axis=1)
            both = jnp.dot(probs[j // 2], v2, preferred_element_type=F32)
            for i in range(2):
                obuf[first + j + i] = both[8 * i:8 * (i + 1), head_dim * i:head_dim * (i + 1)]
        for copy in cache_back(blk):
            copy.start()
        return carry

    lax.fori_loop(0, n_blocks, block_step, 0)
    for h in range(heads):
        out_ref[:, h * head_dim:(h + 1) * head_dim] = obuf[:, h, :].astype(BF16)
    for blk in range(n_blocks):
        for copy in cache_back(blk):
            copy.wait()


def attention(resid_in, positions, k_cache, v_cache, gain_attn, w_query, w_key, w_value):
    rows, width = resid_in.shape
    slots, head_dim = k_cache.shape[1], k_cache.shape[3]
    q_width = w_query.shape[1]
    qkv = q_width + 2 * head_dim
    n_blocks = rows // BLOCK_SEQS
    dma = pltpu.SemaphoreType.DMA
    flat = (rows, slots, head_dim)
    vmem = pl.BlockSpec(memory_space=pltpu.VMEM)
    anywhere = pl.BlockSpec(memory_space=pl.ANY)
    attn_out, k_full, v_full = pl.pallas_call(
        attention_kernel,
        out_shape=(pltpu.VMEM((rows, q_width), BF16),
                   jax.ShapeDtypeStruct(flat, BF16), jax.ShapeDtypeStruct(flat, BF16)),
        in_specs=[anywhere] * 10,
        out_specs=(vmem, anywhere, anywhere),
        scratch_shapes=[
            pltpu.SMEM((rows,), jnp.int32),
            pltpu.VMEM((1, rows), jnp.int32),
            pltpu.VMEM((1, head_dim), F32),
            pltpu.VMEM((width // 128, 128), BF16),
            pltpu.VMEM((rows, width), BF16),
            pltpu.VMEM((rows, width), BF16),
            pltpu.VMEM((width // 128, 128), F32),
            pltpu.VMEM((N_CHUNKS, width // N_CHUNKS, qkv), BF16),
            pltpu.VMEM(flat, BF16),
            pltpu.VMEM(flat, BF16),
            pltpu.VMEM((rows, qkv), F32),
            pltpu.VMEM((rows, 8, head_dim), F32),
            pltpu.VMEM((rows, head_dim), F32),
            pltpu.VMEM((rows, head_dim), F32),
            pltpu.VMEM((rows, 8, head_dim), F32),
            dma((4,)),
            dma(()),
            dma((N_CHUNKS, 3)),
            dma((2, n_blocks)),
            dma((2, n_blocks)),
        ],
        compiler_params=pltpu.CompilerParams(vmem_limit_bytes=64_000_000),
    )(*map(in_hbm, (positions, positions.reshape(1, rows), inverse_frequencies(head_dim),
                    gain_attn.reshape(width // 128, 128), resid_in, w_query, w_key, w_value,
                    k_cache.reshape(flat), v_cache.reshape(flat))))
    return attn_out, k_full.reshape(k_cache.shape), v_full.reshape(v_cache.shape)


REL = ((1, 1), (0, 1), (1, 0), (0, 0))
WO_SLOTS = 4
GU_SLOTS = 5
WD_SLOTS = 4
GATHER_ORDER = ((0, 3), (1, 3), (0, 1), (0, 2), (1, 1), (1, 2), (0, 0), (1, 0))


def flip(coord, do_flip):
    return 1 - coord if do_flip else coord


def tail_kernel(attn_ref, gain_hbm, resid_hbm, wo_hbm, wg_hbm, wu_hbm, wd_hbm, out_ref,
                wo_buf, wg_buf, wu_buf, wd_buf, ybuf, dbuf, r1, r2, xg, acc_g, acc_u, abuf, hbuf,
                resid_buf, stat, stat_out, gain_buf, gbuf, rbuf,
                wo_sem, gu_sem, wd_sem, resid_sem, gain_sem, d_send, d_recv, rs_send, rs_recv,
                ag_send, ag_recv, st_send, st_recv):
    rows = attn_ref.shape[0]
    half = rows // 2
    block = wo_buf.shape[2]
    piece = block // 2
    width = 8 * block

    tp = lax.axis_index('tp')
    core = tp % 2
    x_pos = (tp // 2) % 2
    y_pos = tp // 4

    def device(flip_core, rel):
        flip_y, flip_x = rel
        return flip(y_pos, flip_y) * 4 + flip(x_pos, flip_x) * 2 + flip(core, flip_core)

    def owner(flip_core, e):
        return device(flip_core, REL[e])

    def cols(o):
        return pl.ds(pl.multiple_of(o * block, block), block)

    me = owner(0, 3)
    dev_d = owner(1, 3)
    dev_x = owner(0, 1)
    dev_y = owner(0, 2)

    def remote(src, dst, send, recv, dev):
        return pltpu.make_async_remote_copy(src_ref=src, dst_ref=dst, send_sem=send, recv_sem=recv,
                                            device_id={'tp': dev}, device_id_type=pl.DeviceIdType.MESH)

    order_cols = [(1 - t % 2, t // 2) for t in range(8)]

    def wo_copy(t):
        o = owner(*order_cols[t])
        return pltpu.make_async_copy(wo_hbm.at[:, cols(o)], wo_buf.at[t % WO_SLOTS], wo_sem.at[t % WO_SLOTS])

    def gu_copies(k):
        o = owner(*GATHER_ORDER[k])
        s = k % GU_SLOTS
        return (pltpu.make_async_copy(wg_hbm.at[cols(o), :], wg_buf.at[s], gu_sem.at[0, s]),
                pltpu.make_async_copy(wu_hbm.at[cols(o), :], wu_buf.at[s], gu_sem.at[1, s]))

    def wd_copy(t):
        o = owner(*order_cols[t])
        return pltpu.make_async_copy(wd_hbm.at[:, cols(o)], wd_buf.at[t % WD_SLOTS], wd_sem.at[t % WD_SLOTS])

    for t in range(WO_SLOTS):
        wo_copy(t).start()
    resid_copy = pltpu.make_async_copy(resid_hbm.at[:, cols(me)], resid_buf, resid_sem)
    resid_copy.start()
    gain_copy = pltpu.make_async_copy(gain_hbm, gain_buf, gain_sem)
    gain_copy.start()

    barrier = pltpu.get_barrier_semaphore()
    for j in range(1, 8):
        pl.semaphore_signal(barrier, inc=1, device_id={'tp': (tp + j) % 8}, device_id_type=pl.DeviceIdType.MESH)

    def store_block(dc, e, res):
        for h in range(2):
            for ab in range(2):
                ybuf[dc, e, h, ab] = res[h * half:(h + 1) * half, ab * piece:(ab + 1) * piece]

    def d2d(e):
        return remote(ybuf.at[1, e], dbuf.at[e], d_send.at[e], d_recv.at[e], dev_d)

    def rs_copy(m, h):
        src, dst, dev = (
            (ybuf.at[0, 0, h, 0], r1.at[0, 0, h], dev_x),
            (ybuf.at[0, 1, h, 0], r1.at[0, 1, h], dev_x),
            (ybuf.at[0, 1, h, 1], r2.at[1, h], dev_x),
            (ybuf.at[0, 0, h, 1], r1.at[1, 0, h], dev_y),
            (ybuf.at[0, 2, h, 1], r1.at[1, 1, h], dev_y),
            (ybuf.at[0, 2, h, 0], r2.at[0, h], dev_y),
        )[m]
        return remote(src, dst, rs_send.at[m, h], rs_recv.at[m, h], dev)

    def add_partner(e):
        d2d(e).wait_recv()
        for h in range(2):
            for ab in range(2):
                ybuf[0, e, h, ab] = ybuf[0, e, h, ab] + dbuf[e, h, ab]
            if e == 0:
                rs_copy(0, h).start()
                rs_copy(3, h).start()
            if e == 1:
                rs_copy(1, h).start()
            if e == 2:
                rs_copy(4, h).start()

    def ag_copy(m, h):
        ox, oy, oxy = owner(0, 1), owner(0, 2), owner(0, 0)
        ref, dev = (
            (xg.at[me, h], dev_x),
            (xg.at[me, h], dev_y),
            (xg.at[me, h], dev_d),
            (xg.at[oy, h, 0], dev_x),
            (xg.at[ox, h, 1], dev_y),
            (xg.at[ox, h], dev_d),
            (xg.at[oy, h], dev_d),
            (xg.at[oxy, h, 0], dev_d),
            (xg.at[oxy, h, 1], dev_d),
        )[m]
        return remote(ref, ref, ag_send.at[m, h], ag_recv.at[m, h], dev)

    def reduce_scatter_rest(residual, before_last=None):
        for h in range(2):
            rs_copy(3, h).wait_recv()
            ybuf[0, 1, h, 1] = ybuf[0, 1, h, 1] + r1[1, 0, h]
            rs_copy(2, h).start()
            rs_copy(0, h).wait_recv()
            ybuf[0, 2, h, 0] = ybuf[0, 2, h, 0] + r1[0, 0, h]
            rs_copy(5, h).start()
        for h in range(2):
            rs_copy(1, h).wait_recv()
            rs_copy(4, h).wait_recv()
            rs_copy(2, h).wait_recv()
            rs_copy(5, h).wait_recv()
            for ab in range(2):
                total = ybuf[0, 3, h, ab] + r1[ab, 1, h] + r2[ab, h]
                xg[me, h, ab] = (residual(h, ab) + total).astype(BF16).astype(F32)
            if h == 1 and before_last is not None:
                before_last()
            for m in range(3):
                ag_copy(m, h).start()

    def wait_rs_sends():
        for e in range(4):
            d2d(e).wait_send()
        for m in range(6):
            for h in range(2):
                rs_copy(m, h).wait_send()

    def wait_ag_sends():
        for m in range(9):
            for h in range(2):
                ag_copy(m, h).wait_send()

    def got(m, h):
        ag_copy(m, h).wait_recv()

    def forward_first(h):
        got(0, h)
        got(1, h)
        for m in (3, 4, 5, 6):
            ag_copy(m, h).start()

    def forward_second(h):
        got(3, h)
        ag_copy(7, h).start()
        got(4, h)
        ag_copy(8, h).start()

    attn = attn_ref[...]
    for t in range(8):
        dc, e = order_cols[t]
        wo_copy(t).wait()
        store_block(dc, e, jnp.dot(attn, wo_buf[t % WO_SLOTS], preferred_element_type=F32))
        if t + WO_SLOTS < 8:
            wo_copy(t + WO_SLOTS).start()
        elif t - WO_SLOTS < GU_SLOTS:
            for copy in gu_copies(t - WO_SLOTS):
                copy.start()
        if t == 0:
            pl.semaphore_wait(barrier, 7)
        if dc == 1:
            d2d(e).start()
        elif e >= 1:
            add_partner(e - 1)
    for k in range(8 - WO_SLOTS, GU_SLOTS):
        for copy in gu_copies(k):
            copy.start()
    for t in range(WD_SLOTS):
        wd_copy(t).start()
    add_partner(3)
    resid_copy.wait()
    gain_copy.wait()
    gbuf[...] = gain_buf[...].astype(F32)

    def st_copy(j):
        return remote(stat_out, stat.at[j], st_send.at[j], st_recv.at[j], (tp + j) % 8)

    def send_row_sums():
        parts = []
        for h in range(2):
            sq = jnp.zeros((half, 1), F32)
            for ab in range(2):
                vals = xg[me, h, ab]
                sq = sq + jnp.sum(vals * vals, axis=-1, keepdims=True)
            parts.append(sq)
        sq = jnp.concatenate(parts, axis=0)
        stat_out[...] = jnp.transpose(jnp.broadcast_to(sq, (rows, 128)))[:8]
        for j in range(1, 8):
            st_copy(j).start()

    def read_row_scales():
        sq_all = stat_out[...]
        for j in range(1, 8):
            st_copy(j).wait_recv()
            sq_all = sq_all + stat[j]
        scale = lax.rsqrt(sq_all * (1.0 / width) + EPS)
        rbuf[...] = jnp.transpose(jnp.broadcast_to(scale[:1], (128, rows)))

    reduce_scatter_rest(lambda h, ab: resid_buf[h * half:(h + 1) * half, ab * piece:(ab + 1) * piece].astype(F32),
                        send_row_sums)

    def gate_up(k):
        o = owner(*GATHER_ORDER[k])
        for h in range(2):
            r_half = rbuf[h * half:(h + 1) * half, :]
            for ab in range(2):
                for j in range(piece // 128):
                    gain = gbuf[pl.ds(o * (block // 128) + ab * (piece // 128) + j, 1), :]
                    hbuf[h * half:(h + 1) * half, ab * piece + j * 128:ab * piece + (j + 1) * 128] = (
                        xg[o, h, ab, :, j * 128:(j + 1) * 128] * r_half * gain).astype(BF16)
        s = k % GU_SLOTS
        for copy in gu_copies(k):
            copy.wait()
        normed = hbuf[...]
        gate = jnp.dot(normed, wg_buf[s], preferred_element_type=F32)
        up = jnp.dot(normed, wu_buf[s], preferred_element_type=F32)
        if k == 0:
            acc_g[...] = gate
            acc_u[...] = up
        else:
            acc_g[...] += gate
            acc_u[...] += up
        if k + GU_SLOTS < 8:
            for copy in gu_copies(k + GU_SLOTS):
                copy.start()

    forward_first(0)
    read_row_scales()
    gate_up(0)
    got(2, 0)
    got(2, 1)
    gate_up(1)
    forward_first(1)
    gate_up(2)
    gate_up(3)
    for h in range(2):
        got(5, h)
        got(6, h)
    gate_up(4)
    forward_second(0)
    gate_up(5)
    forward_second(1)
    gate_up(6)
    for h in range(2):
        got(7, h)
        got(8, h)
    gate_up(7)

    gate = acc_g[...].astype(BF16).astype(F32)
    up = acc_u[...].astype(BF16).astype(F32)
    abuf[...] = (jax.nn.silu(gate) * up).astype(BF16)

    wait_rs_sends()
    wait_ag_sends()
    for t in range(8):
        dc, e = order_cols[t]
        wd_copy(t).wait()
        store_block(dc, e, jnp.dot(abuf[...], wd_buf[t % WD_SLOTS], preferred_element_type=F32))
        if t + WD_SLOTS < 8:
            wd_copy(t + WD_SLOTS).start()
        if dc == 1:
            d2d(e).start()
        elif e >= 1:
            add_partner(e - 1)
    add_partner(3)
    reduce_scatter_rest(lambda h, ab: xg[me, h, ab])

    def write_out(k):
        o = owner(*GATHER_ORDER[k])
        for h in range(2):
            for ab in range(2):
                out_ref[h * half:(h + 1) * half, pl.ds(pl.multiple_of(o * block + ab * piece, 128), piece)] = (
                    xg[o, h, ab].astype(BF16))

    write_out(0)
    got(2, 0)
    got(2, 1)
    write_out(1)
    forward_first(0)
    forward_first(1)
    write_out(2)
    write_out(3)
    forward_second(0)
    for h in range(2):
        got(5, h)
        got(6, h)
    write_out(4)
    write_out(5)
    forward_second(1)
    write_out(6)
    for h in range(2):
        got(7, h)
        got(8, h)
    write_out(7)
    for j in range(1, 8):
        st_copy(j).wait_send()
    wait_rs_sends()
    wait_ag_sends()


def mlp_tail(attn_out, resid_in, gain_mlp, w_out, w_gate, w_up, w_down):
    rows, width = resid_in.shape
    depth = w_out.shape[0]
    ffn = w_gate.shape[1]
    block = width // 8
    piece = block // 2
    half = rows // 2
    dma = pltpu.SemaphoreType.DMA
    return pl.pallas_call(
        tail_kernel,
        out_shape=pltpu.VMEM((rows, width), BF16),
        in_specs=[pl.BlockSpec(memory_space=pltpu.VMEM)] + [pl.BlockSpec(memory_space=pl.ANY)] * 6,
        out_specs=pl.BlockSpec(memory_space=pltpu.VMEM),
        scratch_shapes=[
            pltpu.VMEM((WO_SLOTS, depth, block), BF16),
            pltpu.VMEM((GU_SLOTS, block, ffn), BF16),
            pltpu.VMEM((GU_SLOTS, block, ffn), BF16),
            pltpu.VMEM((WD_SLOTS, ffn, block), BF16),
            pltpu.VMEM((2, 4, 2, 2, half, piece), F32),
            pltpu.VMEM((4, 2, 2, half, piece), F32),
            pltpu.VMEM((2, 2, 2, half, piece), F32),
            pltpu.VMEM((2, 2, half, piece), F32),
            pltpu.VMEM((8, 2, 2, half, piece), F32),
            pltpu.VMEM((rows, ffn), F32),
            pltpu.VMEM((rows, ffn), F32),
            pltpu.VMEM((rows, ffn), BF16),
            pltpu.VMEM((rows, block), BF16),
            pltpu.VMEM((rows, block), BF16),
            pltpu.VMEM((8, 8, rows), F32),
            pltpu.VMEM((8, rows), F32),
            pltpu.VMEM((width // 128, 128), BF16),
            pltpu.VMEM((width // 128, 128), F32),
            pltpu.VMEM((rows, 128), F32),
            dma((WO_SLOTS,)),
            dma((2, GU_SLOTS)),
            dma((WD_SLOTS,)),
            dma(()),
            dma(()),
            dma((4,)),
            dma((4,)),
            dma((6, 2)),
            dma((6, 2)),
            dma((9, 2)),
            dma((9, 2)),
            dma((8,)),
            dma((8,)),
        ],
        compiler_params=pltpu.CompilerParams(collective_id=0, has_side_effects=True,
                                             vmem_limit_bytes=64_500_000),
    )(in_vmem(attn_out), *map(in_hbm, (gain_mlp.reshape(width // 128, 128), resid_in, w_out, w_gate, w_up, w_down)))


def write_kernel(resid_ref, resid_hbm, sem):
    copy = pltpu.make_async_copy(resid_ref, resid_hbm, sem)
    copy.start()
    copy.wait()


def write_back(resid_out):
    return pl.pallas_call(
        write_kernel,
        out_shape=jax.ShapeDtypeStruct(resid_out.shape, resid_out.dtype),
        in_specs=[pl.BlockSpec(memory_space=pltpu.VMEM)],
        out_specs=pl.BlockSpec(memory_space=pl.ANY),
        scratch_shapes=[pltpu.SemaphoreType.DMA(())],
    )(in_vmem(resid_out))


def solution(mesh):
    def layer_local(resid_in, positions, k_cache, v_cache, gain_attn, w_query, w_key, w_value,
                    w_out, gain_mlp, w_gate, w_up, w_down):
        attn_out, k_full, v_full = attention(resid_in, positions, k_cache, v_cache, gain_attn,
                                             w_query, w_key, w_value)
        resid_out = mlp_tail(attn_out, resid_in, gain_mlp, w_out, w_gate, w_up, w_down)
        return write_back(resid_out), k_full, v_full

    row_spec = P('dp', None)
    cache_spec = P('dp', None, 'tp', None)
    col_spec = P(None, 'tp')
    split_rows = P('tp', None)
    return jax.shard_map(layer_local, mesh=mesh,
                         in_specs=(row_spec, P('dp'), cache_spec, cache_spec, P(), col_spec, col_spec,
                                   col_spec, split_rows, P(), col_spec, col_spec, split_rows),
                         out_specs=(row_spec, cache_spec, cache_spec), check_vma=False)
```
